32 devices in a mesh: pair: 8 (over z, x), aux: 4 (over y, core).
Axes of the slice: x: 2, y: 2, z: 4, core: 2. Of those that a mesh axis runs over, the one named last changes fastest.
Arguments:
- panels: bfloat16 [16, 120, 9216], P('pair', None, 'aux'), may hold values from -1.5 to 1.5
- amplitudes: bfloat16 [16, 2, 120, 120], P('pair'), may hold values from -0.5 to 0.5
- drive: float32 [16, 2, 14400], P('pair', None, 'aux'), may hold values from -6 to 6
- pno_energy: float32 [16, 120], P('pair'), may hold values from 1 to 3
- occ_energy: float32 [32], replicated, may hold values from -2 to -0.5
- frequency: float32 [1], replicated, may hold values from 0.2 to 2
- pair_lmo: int32 [16, 2], replicated, may hold values from 0 to 31
- neighbours: int32 [16, 8], P('pair'), may hold values from 0 to 15
- pno_ranks: int32 [16], P('pair'), may hold values from 60 to 120
- fock_off: float32 [32, 32], replicated, may hold values from -1.8 to 1.8
Outputs:
- residual: float32 [16, 2, 14400], P('pair', None, 'aux')
The draws below stay inside these ranges and needn't reach their ends.
Inputs may be any that keep to these rules, and one draw needn't show every extreme that they name: `neighbours`: neighbour pairs; a pair may be listed more than once and may list itself. `pno_ranks`: rows of a pair's panel from its rank on are padding.
All inputs are finite; a program needn't handle non-finite values.
Results may differ from the reference program's by a relative error of at most 0.0033.
Values may be sent and summed in bfloat16 or wider, within the bound.
A program may use at most 128 MiB of HBM per device.

```python
import jax
import jax.numpy as jnp
from jax import lax

R = 120
AUX_DEV = 2304
AUX = 9216
PAIRS = 16
NBR = 8
NLMO = 32
RR = 14400
N_AUX = 4


def plant(values, rng, least, high):
    longest = values.shape.index(max(values.shape))
    spots = []
    for shift in (0, 1):
        where = [jax.random.randint(jax.random.fold_in(rng, axis), (), 0, length) for axis, length in enumerate(values.shape)]
        where[longest] = (where[longest] + shift) % values.shape[longest]
        spots.append(tuple(where))
    return values.at[spots[0]].set(least).at[spots[1]].set(high)


def levels(own_key, shape, pieces, least, largest):
    def one(axis_at, shards_of):
        draws = jax.random.uniform(jax.random.fold_in(jax.random.fold_in(own_key, 6), axis_at), (shards_of,), jnp.float32, least / len(pieces), largest / len(pieces))
        return jnp.repeat(jnp.exp(draws), shape[axis_at] // shards_of).reshape((-1,) + (1,) * (len(shape) - axis_at - 1))

    loudness = one(*pieces[0])
    for cut in pieces[1:]:
        loudness = loudness * one(*cut)
    return loudness


def bell_draw(rng, dims, width, reach, split=(), kind=jnp.bfloat16):
    entries = jax.random.normal(rng, dims, jnp.float32) * width
    if len(split) > 0:
        entries = levels(rng, dims, split, -0.22, 0.18) * entries
    return jnp.clip(entries, min=-reach, max=reach).astype(kind)


def setup_inputs(seed: int = 0) -> dict:
    splits = jax.random.split(jax.random.key(seed), 11)
    return {
        "panels": bell_draw(splits[0], (PAIRS, R, AUX), (AUX ** -0.25), 1.5, ((0, 8), (2, 4))),
        "amplitudes": bell_draw(splits[1], (PAIRS, 2, R, R), R ** -0.5, 0.5, ((0, 8),)),
        "drive": bell_draw(splits[2], (PAIRS, 2, RR), 1.0, 6.0, ((0, 8), (2, 4)), jnp.float32),
        "pno_energy": jnp.clip(1.0 + 2.0 * jax.random.uniform(splits[3], (PAIRS, R), jnp.float32) ** levels(splits[3], (PAIRS, R), ((0, 8),), -0.2, 0.2), 1.0, 3.0),
        "occ_energy": jnp.clip(jax.random.uniform(splits[4], (NLMO,), jnp.float32, -2.0, -0.5), -2.0, -0.5),
        "frequency": jnp.clip(jax.random.uniform(splits[5], (1,), jnp.float32, 0.2, 2.0), 0.2, 2.0),
        "pair_lmo": plant(jax.random.randint(splits[6], (PAIRS, 2), 0, NLMO), jax.random.fold_in(splits[6], 1), 0, NLMO - 1).astype(jnp.int32),
        "neighbours": plant(jax.random.randint(splits[7], (PAIRS, NBR), 0, PAIRS), jax.random.fold_in(splits[7], 1), 0, PAIRS - 1).astype(jnp.int32),
        "pno_ranks": plant(jax.random.randint(splits[8], (PAIRS,), R // 2, R + 1), jax.random.fold_in(splits[8], 1), R // 2, R).astype(jnp.int32),
        "fock_off": bell_draw(splits[9], (NLMO, NLMO), 0.3, 1.8, (), jnp.float32),
    }


def reference(panels, amplitudes, drive, pno_energy, occ_energy, frequency, pair_lmo, neighbours, pno_ranks, fock_off):
    rows_index = jnp.arange(R, dtype=jnp.int32)
    keep_rows = rows_index[None, :] < pno_ranks[:, None]
    masked = jnp.where(keep_rows[:, :, None], panels, jnp.zeros_like(panels))
    near_lmo = pair_lmo[neighbours]
    values = fock_off[pair_lmo[:, 0][:, None], near_lmo[:, :, 0]] + fock_off[pair_lmo[:, 1][:, None], near_lmo[:, :, 1]]
    onehot = (neighbours[:, :, None] == jnp.arange(PAIRS, dtype=jnp.int32)[None, None, :]).astype(jnp.float32)
    weights = jnp.sum(values[:, :, None] * onehot, axis=1).astype(jnp.bfloat16)
    weights_wide = weights.astype(jnp.float32)
    matrices = jnp.transpose(amplitudes, (0, 2, 1, 3)).reshape(PAIRS, R, 2 * R).astype(jnp.float32)

    def block_step(running_sum, block_index):
        start_col = (block_index * AUX_DEV).astype(jnp.int32)
        slab = lax.dynamic_slice_in_dim(masked, start_col, AUX_DEV, 2).astype(jnp.float32)
        projected = jnp.einsum('nra,nrc->nac', slab, matrices, precision=lax.Precision.HIGHEST).astype(jnp.bfloat16)
        projected = lax.optimization_barrier(projected).astype(jnp.float32)
        collected = jnp.einsum('pn,nac->pac', weights_wide, projected, precision=lax.Precision.HIGHEST).astype(jnp.bfloat16)
        collected = lax.optimization_barrier(collected).astype(jnp.float32)
        running_sum = running_sum + jnp.einsum('pra,pac->prc', slab, collected, precision=lax.Precision.HIGHEST)
        return running_sum, None

    start_sum = jnp.zeros((PAIRS, R, 2 * R), jnp.float32)
    coupled, unused_out = lax.scan(block_step, start_sum, jnp.arange(N_AUX, dtype=jnp.int32))
    coupled = jnp.transpose(coupled.reshape(PAIRS, R, 2, R), (0, 2, 1, 3))
    occ_pair = occ_energy[pair_lmo[:, 0]] + occ_energy[pair_lmo[:, 1]]
    shift = pno_energy[:, :, None] + pno_energy[:, None, :] - occ_pair[:, None, None]
    signs = jnp.array([1.0, -1.0], jnp.float32)
    factor = shift[:, None, :, :] - signs[None, :, None, None] * frequency[0]
    diagonal_term = factor * amplitudes.astype(jnp.float32)
    return drive + diagonal_term.reshape(PAIRS, 2, R * R) + coupled.reshape(PAIRS, 2, R * R)
```

```python
import functools

import jax
import jax.numpy as jnp
from jax import lax
from jax.experimental import pallas as pl
from jax.experimental.pallas import tpu as pltpu
from jax.sharding import PartitionSpec as P

LANE = 128


def pair_weights(pair_lmo, neighbours, fock_off, first_pair):
    local_pairs = neighbours.shape[0]
    total_pairs = pair_lmo.shape[0]
    lmo_count = fock_off.shape[0]
    lmo_ids = jnp.arange(lmo_count, dtype=jnp.int32)
    own_lmo = lax.dynamic_slice_in_dim(pair_lmo, first_pair, local_pairs, 0)
    own_table = (own_lmo[:, :, None] == lmo_ids[None, None, :]).astype(jnp.float32)
    lmo_table = (pair_lmo[:, :, None] == lmo_ids[None, None, :]).astype(jnp.float32)
    pair_ids = jnp.arange(total_pairs, dtype=jnp.int32)
    onehot = (neighbours[:, :, None] == pair_ids[None, None, :]).astype(jnp.float32)
    fock_rows = jnp.einsum("psl,lm->psm", own_table, fock_off, precision=lax.Precision.HIGHEST)
    near_table = jnp.einsum("pkn,nsl->pksl", onehot, lmo_table)
    values = jnp.sum(fock_rows[:, None, :, :] * near_table, axis=(2, 3))
    weights = jnp.sum(values[:, :, None] * onehot, axis=1).astype(jnp.bfloat16)
    return (weights, own_table)


def plain_body(
    panels,
    amplitudes,
    drive,
    pno_energy,
    occ_energy,
    frequency,
    pair_lmo,
    neighbours,
    pno_ranks,
    fock_off,
):
    local_pairs, rank_dim, aux_width = panels.shape
    total_pairs = pair_lmo.shape[0]
    n_pair = lax.axis_size("pair")
    n_aux = lax.axis_size("aux")
    first_pair = lax.axis_index("pair") * local_pairs
    rows_index = jnp.arange(rank_dim, dtype=jnp.int32)
    keep_rows = rows_index[None, :] < pno_ranks[:, None]
    weights, own_table = pair_weights(pair_lmo, neighbours, fock_off, first_pair)
    weights = lax.all_gather(weights, "pair", axis=0, tiled=True)
    amps = jnp.where(keep_rows[:, :, None, None], jnp.transpose(amplitudes, (0, 2, 1, 3)), 0)
    amps = lax.all_gather(
        amps.reshape(local_pairs * rank_dim, 2 * rank_dim), "pair", axis=0, tiled=True
    )
    masked = jnp.where(keep_rows[:, :, None], panels, jnp.zeros_like(panels))
    slices = lax.all_to_all(
        masked.reshape(local_pairs * rank_dim, aux_width), "pair", 1, 0, tiled=True
    )
    products = jnp.einsum("iq,jq->ij", slices, slices, preferred_element_type=jnp.float32)
    products = products.reshape(total_pairs, rank_dim, total_pairs, rank_dim)
    mixed = (products * weights.astype(jnp.float32)[:, None, :, None]).astype(jnp.bfloat16)
    mixed = mixed.reshape(total_pairs * rank_dim, total_pairs * rank_dim)
    coupled = jnp.dot(mixed, amps, preferred_element_type=jnp.float32).astype(jnp.bfloat16)
    share_width = drive.shape[2]
    coupled = coupled.reshape(total_pairs, rank_dim, 2, rank_dim).transpose(0, 2, 1, 3)
    coupled = coupled.reshape(n_pair, local_pairs, 2, n_aux, share_width).transpose(0, 3, 1, 2, 4)
    coupled = coupled.reshape(n_pair * n_aux, local_pairs, 2, share_width)
    coupled = lax.all_to_all(coupled, ("pair", "aux"), 0, 0, tiled=True)
    coupled_share = jnp.sum(coupled.astype(jnp.float32), axis=0)
    share_start = lax.axis_index("aux") * share_width
    occ_pair = jnp.sum(own_table * occ_energy[None, None, :], axis=(1, 2))
    shift = pno_energy[:, :, None] + pno_energy[:, None, :] - occ_pair[:, None, None]
    shift_flat = lax.dynamic_slice_in_dim(
        shift.reshape(local_pairs, rank_dim * rank_dim), share_start, share_width, 1
    )
    signs = jnp.array([1.0, -1.0], jnp.float32)
    factor = shift_flat[:, None, :] - signs[None, :, None] * frequency[0]
    amp_flat = amplitudes.reshape(local_pairs, 2, rank_dim * rank_dim)
    amp_share = lax.dynamic_slice_in_dim(amp_flat, share_start, share_width, 2).astype(jnp.float32)
    return drive + factor * amp_share + coupled_share


def remote(src, dst, send_sem, recv_sem, pair, aux):
    return pltpu.make_async_remote_copy(
        src_ref=src,
        dst_ref=dst,
        send_sem=send_sem,
        recv_sem=recv_sem,
        device_id=(pair, aux),
        device_id_type=pl.DeviceIdType.MESH,
    )


def kernel(
    n_pair, n_aux, rank, x_hbm, amp_hbm, energy_hbm, fock_hbm,
    occ_ref, frequency_ref, lmo_ref, neighbour_ref, rank_ref, out_ref,
    xv, amp_v, energy_v, fock_v, a_ref, term, xb, ab, wt, left_rows, acc, parts, parts_in, ends, ends_in,
    load_sem, small_sem, local_sem,
    x_send, x_recv, e_send, e_recv, f_send, f_recv, g_send, g_recv,
    a_send, a_recv, b_send, b_recv, p_send, p_recv, q_send, q_recv,
):
    me = lax.axis_index("pair")
    aux = lax.axis_index("aux")
    core = lax.rem(aux, 2)
    chip = aux // 2
    mate = aux + 1 - 2 * core
    n_chip = n_aux // 2
    block = 2 * rank
    tiles = xv.shape[1] // LANE
    base = (tiles // n_pair) * LANE
    extra = tiles % n_pair
    stride = n_pair // (2 * extra) if extra else 1
    share = a_ref.shape[0] // n_aux
    quarter = rank // n_aux
    padded = ends_in.shape[2]
    half = n_pair // 2
    near = (me // half) * half
    far = half - near
    spot_me = me - near
    across = far + spot_me

    loads = load_sem.shape[0]
    piece = xv.shape[1] // loads

    def load_x(s):
        lanes = pl.ds(s * piece, piece)
        return pltpu.make_async_copy(x_hbm.at[:, lanes], xv.at[:, lanes], load_sem.at[s])

    smalls = [
        pltpu.make_async_copy(amp_hbm, amp_v, small_sem.at[0]),
        pltpu.make_async_copy(fock_hbm, fock_v, small_sem.at[1]),
        pltpu.make_async_copy(energy_hbm, energy_v, small_sem.at[2]),
    ]
    for copy in smalls:
        copy.start()
    for s in range(loads):
        load_x(s).start()

    barrier = pltpu.get_barrier_semaphore()

    def greet(pair, other):
        pl.semaphore_signal(
            barrier, inc=1, device_id=(pair, other), device_id_type=pl.DeviceIdType.MESH
        )

    def near_peer(t):
        return near + lax.rem(spot_me + t, half)

    def far_peer(t):
        return far + lax.rem(spot_me + t, half)

    def row(u):
        return 2 * lax.rem(chip + u, n_chip) + core

    for t in range(half):
        greet(far_peer(t), aux)
    for t in range(1, half):
        greet(near_peer(t), aux)
        for u in range(1, n_chip):
            greet(near_peer(t), row(u))
    greet(across, mate)
    for t in range(1, n_aux):
        greet(me, lax.rem(aux + t, n_aux))

    def holder(which, level):
        spot = 2 * level + which
        shift = spot % 2 if not hasattr(spot, "dtype") else lax.rem(spot, 2)
        return stride * spot + (shift if stride > 1 else 0)

    lanes = pl.ds(pl.multiple_of(core * base, LANE), base)
    mate_lanes = pl.ds(pl.multiple_of((1 - core) * base, LANE), base)
    extra_lanes = pl.ds(2 * base, LANE)
    my_share = pl.ds(pl.multiple_of(aux * share, 16), share)

    def own_cols(peer):
        return xv.at[:, pl.ds(pl.multiple_of(peer * base, LANE), base)]

    def send_a(t):
        peer = near_peer(t) if t else across
        return remote(a_ref.at[my_share], ab.at[me, my_share], a_send.at[t], a_recv.at[me], peer, aux)

    def pass_a(t):
        rows = ab.at[across, my_share]
        return remote(rows, rows, a_send.at[half + t], a_recv.at[across], near_peer(t), aux)

    def wait_a(j):
        remote(
            a_ref.at[my_share], ab.at[j, my_share], a_send.at[0], a_recv.at[j], me, mate
        ).wait_recv()

    def send_x(peer):
        return remote(
            own_cols(peer), xb.at[me, :, lanes], x_send.at[peer], x_recv.at[me], peer, aux
        )

    def wait_x(j):
        remote(
            own_cols(me), xb.at[j, :, lanes], x_send.at[j], x_recv.at[j], me, mate
        ).wait_recv()

    def wait_f(j):
        remote(
            own_cols(me), xb.at[j, :, mate_lanes], f_send.at[j], f_recv.at[j], me, mate
        ).wait_recv()

    def extra_cols(level):
        return xv.at[:, pl.ds(base * n_pair + level * LANE, LANE)]

    def send_e(level):
        return remote(
            extra_cols(level), xb.at[me, :, extra_lanes], e_send.at[level], e_recv.at[me],
            holder(core, level), aux,
        )

    def send_f(j):
        return remote(xb.at[j, :, lanes], xb.at[j, :, lanes], f_send.at[j], f_recv.at[j], me, mate)

    def own_f():
        return remote(own_cols(me), xb.at[me, :, lanes], f_send.at[me], f_recv.at[me], me, mate)

    def send_g(j):
        return remote(
            xb.at[j, :, extra_lanes], xb.at[j, :, extra_lanes], g_send.at[j], g_recv.at[j], me, mate
        )

    def send_b(j, u):
        rows = ab.at[j, my_share]
        return remote(rows, rows, b_send.at[j, u], b_recv.at[aux, j], me, lax.rem(aux + u, n_aux))

    mine_x = pltpu.make_async_copy(own_cols(me), xb.at[me, :, lanes], local_sem.at[0])
    mine_a = pltpu.make_async_copy(a_ref, ab.at[me], local_sem.at[1])

    def holds(which):
        found = me < 0
        for level in range(extra):
            found = jnp.logical_or(found, holder(which, level) == me)
        return found

    self_holds = holds(core)
    mate_holds = holds(1 - core)
    if extra:
        @pl.when(jnp.logical_not(jnp.logical_or(self_holds, mate_holds)))
        def _():
            xb[:, :, 2 * base :] = jnp.zeros((n_pair, block, LANE), xb.dtype)

    for copy in smalls:
        copy.wait()
    own_amplitudes(rank, me, amp_v, fock_v, lmo_ref, neighbour_ref, rank_ref, a_ref)
    mine_a.start()
    for s in range(loads):
        load_x(s).wait()
    pl.semaphore_wait(barrier, n_pair + (half - 1) * (n_chip - 1) + n_aux - 1)

    for t in range(half):
        send_a(t).start()
    for level in range(extra):
        @pl.when(holder(core, level) != me)
        def _():
            send_e(level).start()

        @pl.when(holder(core, level) == me)
        def _():
            pltpu.make_async_copy(
                extra_cols(level), xb.at[me, :, extra_lanes], local_sem.at[2]
            ).start()
    level = me // (half // 2)
    inner = jnp.logical_or(level == 1, level == 2)

    @pl.when(inner)
    def _():
        for t in range(half):
            send_x(far_peer(t)).start()

    own_f().start()
    mine_x.start()
    own_term(rank, n_aux, me, aux, amp_v, energy_v, occ_ref, frequency_ref, lmo_ref, term)

    wait_a(across)
    for t in range(1, half):
        pass_a(t).start()
    for u in range(1, n_aux):
        send_b(across, u).start()
    for t in range(1, half):
        send_x(near_peer(t)).start()

    @pl.when(jnp.logical_not(inner))
    def _():
        for t in range(half):
            send_x(far_peer(t)).start()

    for t in range(1, half):
        j = near_peer(half - t)
        wait_a(j)
        for u in range(1, n_aux):
            send_b(j, u).start()
    for t in range(1, half):
        j = far_peer(half - t)
        wait_a(j)
        for u in range(1, n_aux):
            send_b(j, u).start()
    mine_x.wait()
    mine_a.wait()
    if extra:
        @pl.when(self_holds)
        def _():
            pltpu.make_async_copy(
                extra_cols(0), xb.at[me, :, extra_lanes], local_sem.at[2]
            ).wait()
            send_g(me).start()
            for t in range(1, n_pair):
                j = lax.rem(me + n_pair - t, n_pair)
                remote(
                    extra_cols(0), xb.at[j, :, extra_lanes], e_send.at[0], e_recv.at[j], me, mate
                ).wait_recv()
                send_g(j).start()

        @pl.when(mate_holds)
        def _():
            for j in range(n_pair):
                send_g(j).wait_recv()
    for t in range(1, half):
        j = near_peer(half - t)
        wait_x(j)
        send_f(j).start()
    for t in range(1, n_pair):
        j = lax.rem(me + n_pair - t, n_pair)
        for u in range(1, n_aux):
            other = lax.rem(aux + u, n_aux)
            rows = ab.at[j, pl.ds(pl.multiple_of(other * share, 16), share)]
            remote(rows, rows, b_send.at[j, u], b_recv.at[other, j], me, other).wait_recv()

    rows = [ab[j, block : block + 16, :LANE].astype(jnp.float32) for j in range(n_pair)]
    rows = [jnp.where(core == 0, r[0:1], r[1:2]) for r in rows]
    table = jnp.concatenate(rows, axis=0).astype(jnp.bfloat16)
    pair_row = lax.broadcasted_iota(jnp.int32, (LANE, block), 0)
    column = lax.broadcasted_iota(jnp.int32, (LANE, block), 1)
    for j in range(n_pair):
        pick = pair_row == jnp.where(column < rank, 2 * j, 2 * j + 1)
        pick = jnp.where(pick, 1.0, 0.0).astype(jnp.bfloat16)
        wt[j] = jnp.dot(table, pick, preferred_element_type=jnp.float32)

    def collect_rows(i):
        for side in range(2):
            @pl.when(core == side)
            def _():
                left_rows[i] = xb[i, side * rank : (side + 1) * rank, :]

    def join(pieces):
        return jnp.concatenate(pieces, axis=0) if len(pieces) > 1 else pieces[0]

    def turned(indices, blocks):
        rows = join([left_rows[i] for i in indices])
        columns = join([xb[j] for j in blocks])
        products = lax.dot_general(
            rows, columns, (((1,), (1,)), ((), ())), preferred_element_type=jnp.float32
        )
        total = None
        for m, j in enumerate(blocks):
            part = products[:, m * block : (m + 1) * block]
            scaled = [
                part[k * rank : (k + 1) * rank] * wt[j, pl.ds(i, 1), :]
                for k, i in enumerate(indices)
            ]
            turn = jnp.dot(
                join(scaled).astype(jnp.bfloat16), ab[j, :block, :],
                preferred_element_type=jnp.float32,
            )
            total = turn if total is None else total + turn
        return total

    def couple(indices, blocks, first=False):
        turn = turned(indices, blocks)
        for k, i in enumerate(indices):
            rows = turn[k * rank : (k + 1) * rank]
            if first:
                acc[i, :rank, :] = rows
            else:
                acc[i, :rank, :] += rows

    near_all = [near + t for t in range(half)]
    for t in range(half):
        wait_f(near_peer(t))
        collect_rows(near_peer(t))
    for t in range(half):
        couple(near_all, [near + t], first=t == 0)

    def send_p(which, t, u):
        peer = near_peer(t)
        other = lax.rem(chip + u, n_chip)
        i = far_peer(t) if which else peer
        return remote(
            parts.at[i, other], parts_in.at[which, t, u], p_send.at[which, t, u],
            p_recv.at[which, t, u], peer, 2 * other + core,
        )

    hops = [(t, u) for t in range(half) for u in range(n_chip) if t or u]

    def spread(which):
        for t in range(half):
            i = far_peer(t) if which else near_peer(t)
            for k in range(n_aux):
                rows = acc[i, quarter * k : quarter * k + padded, :]
                parts[i, k // 2, (k % 2) * padded : (k % 2 + 1) * padded, :] = rows.astype(
                    parts.dtype
                )
            for u in range(n_chip):
                if t or u:
                    send_p(which, t, u).start()

    for k in range(half):
        e = far_peer((half - k) % half)
        earlier = [far_peer((half - m) % half) for m in range(k)]
        wait_x(e)
        send_f(e).start()
        wait_f(e)
        collect_rows(e)

        couple([e], near_all + earlier + [e], first=True)
        if earlier:
            couple(earlier, [e])
        if k == half - 1:
            spread(1)
        couple(near_all, [e])
    spread(0)

    def collect(which):
        i = across if which else me
        total = parts[i, chip].astype(jnp.float32)
        for t, u in hops:
            send_p(which, t, u).wait_recv()
            total = total + parts_in[which, t, u].astype(jnp.float32)
        ends[which] = total.astype(ends.dtype)

    def send_q(k):
        return remote(
            ends.at[1, pl.ds(k * padded, padded)], ends_in.at[1, core],
            q_send.at[k], q_recv.at[1, core], across, 2 * chip + k,
        )

    def mate_q():
        return remote(
            ends.at[0, pl.ds(pl.multiple_of((1 - core) * padded, padded), padded)],
            ends_in.at[0, core], q_send.at[2], q_recv.at[0, core], me, mate,
        )

    collect(1)
    for k in range(2):
        send_q(k).start()
    collect(0)
    mate_q().start()
    ends_in[0, core] = ends[0, pl.ds(pl.multiple_of(core * padded, padded), padded), :]

    def arrive(which, side):
        remote(
            ends.at[which, pl.ds(0, padded)], ends_in.at[which, side],
            q_send.at[0], q_recv.at[which, side], me, mate,
        ).wait_recv()

    arrive(0, 1 - core)
    for side in range(2):
        arrive(1, side)
        total = ends_in[0, side].astype(jnp.float32) + ends_in[1, side].astype(jnp.float32)
        at = lax.broadcasted_iota(jnp.int32, (padded, LANE), 0) + aux * quarter
        for s in range(2):
            part = total[:, s * LANE : (s + 1) * LANE]
            part = jnp.where(at < rank_ref[side], part, 0.0)
            part = part + term[side, s, pl.ds(aux * quarter, padded), :]
            for r in range(quarter):
                out_ref[side, s : s + 1, r * rank : (r + 1) * rank] = part[r : r + 1, :rank]

    for t in range(half):
        send_a(t).wait_send()
        send_x(far_peer(t)).wait_send()
        if t:
            pass_a(t).wait_send()
            send_x(near_peer(t)).wait_send()
    for t in range(1, n_pair):
        j = lax.rem(me + n_pair - t, n_pair)
        send_f(j).wait_send()
        for u in range(1, n_aux):
            send_b(j, u).wait_send()
    own_f().wait_send()
    for level in range(extra):
        @pl.when(holder(core, level) != me)
        def _():
            send_e(level).wait_send()
    if extra:
        @pl.when(self_holds)
        def _():
            for j in range(n_pair):
                send_g(j).wait_send()
    for which in range(2):
        for t, u in hops:
            send_p(which, t, u).wait_send()
    for k in range(2):
        send_q(k).wait_send()
    mate_q().wait_send()


def own_amplitudes(rank, me, amp_v, fock_v, lmo_ref, neighbour_ref, rank_ref, a_ref):
    total_pairs = lmo_ref.shape[1]
    lmo_count = fock_v.shape[0]
    a_ref[...] = jnp.zeros_like(a_ref)
    at = lax.broadcasted_iota(jnp.int32, (rank, rank), 0)
    for p in range(2):
        for s in range(2):
            part = jnp.where(at < rank_ref[p], amp_v[p, s].astype(jnp.float32), 0.0)
            a_ref[p * rank : (p + 1) * rank, s * LANE : s * LANE + rank] = part.astype(a_ref.dtype)
    lane = lax.broadcasted_iota(jnp.int32, (1, LANE), 1)
    level = lax.broadcasted_iota(jnp.int32, (lmo_count, LANE), 0)
    values = 0.0
    for side in range(2):
        where = jnp.full((1, LANE), -1, jnp.int32)
        for n in range(total_pairs):
            where = jnp.where(lane == n, lmo_ref[side, n], where)
        table = jnp.where(level == where, 1.0, 0.0)
        rows = [fock_v[pl.ds(lmo_ref[side, 2 * me + p], 1), :] for p in range(2)]
        rows = jnp.concatenate(rows + [jnp.zeros((6, lmo_count), jnp.float32)], axis=0)
        values = values + jnp.dot(
            rows, table, preferred_element_type=jnp.float32, precision=lax.Precision.HIGHEST
        )
    counts = []
    for p in range(2):
        count = jnp.zeros((1, LANE), jnp.float32)
        for k in range(neighbour_ref.shape[1]):
            count = count + jnp.where(lane == neighbour_ref[p, k], 1.0, 0.0)
        counts.append(count)
    counts = jnp.concatenate(counts + [jnp.zeros((6, LANE), jnp.float32)], axis=0)
    rows = jnp.concatenate([values * counts, jnp.zeros((8, LANE), jnp.float32)], axis=0)
    a_ref[2 * rank : 2 * rank + 16, :LANE] = rows.astype(a_ref.dtype)


def own_term(rank, n_aux, me, aux, amp_v, energy_v, occ_ref, frequency_ref, lmo_ref, term):
    row = lax.broadcasted_iota(jnp.int32, (rank, rank), 0)
    column = lax.broadcasted_iota(jnp.int32, (rank, rank), 1)
    term[...] = jnp.zeros_like(term)
    for p in range(2):
        energy = jnp.broadcast_to(energy_v[p : p + 1, :], (rank, rank))
        own = jnp.sum(jnp.where(row == column, energy, 0.0), axis=1, keepdims=True)
        pair = 2 * me + p
        occ = occ_ref[lmo_ref[0, pair]] + occ_ref[lmo_ref[1, pair]]
        shift = own + energy - occ
        for s in range(2):
            factor = shift - frequency_ref[0] if s == 0 else shift + frequency_ref[0]
            term[p, s, :rank, :rank] = factor * amp_v[p, s].astype(jnp.float32)


def fused_coupling(
    x_own, amplitudes, energy, fock, occ, frequency, lmo, neighbours, ranks, n_pair, n_aux, rank
):
    block = 2 * rank
    tiles = x_own.shape[1] // LANE
    depth = 2 * (tiles // n_pair) * LANE + (LANE if tiles % n_pair else 0)
    n_chip = n_aux // 2
    half = n_pair // 2
    extra = max(tiles % n_pair, 1)
    wide = 2 * LANE
    a_shape = (-(-(block + 16) // (16 * n_aux)) * 16 * n_aux, wide)
    padded = -(-(rank // n_aux) // 16) * 16
    tall = -(-(rank - rank // n_aux + padded) // 8) * 8
    loads = 2 if tiles % 2 == 0 else 1
    dma = pltpu.SemaphoreType.DMA
    bf16 = jnp.bfloat16
    anywhere = pl.BlockSpec(memory_space=pl.ANY)
    scalars = pl.BlockSpec(memory_space=pltpu.SMEM)
    return pl.pallas_call(
        functools.partial(kernel, n_pair, n_aux, rank),
        out_shape=jax.ShapeDtypeStruct((2, 2, rank // n_aux * rank), jnp.float32),
        in_specs=[anywhere] * 4 + [scalars] * 5,
        out_specs=pl.BlockSpec(memory_space=pltpu.VMEM),
        scratch_shapes=[
            pltpu.VMEM(x_own.shape, bf16),
            pltpu.VMEM(amplitudes.shape, bf16),
            pltpu.VMEM(energy.shape, jnp.float32),
            pltpu.VMEM(fock.shape, jnp.float32),
            pltpu.VMEM(a_shape, bf16),
            pltpu.VMEM((2, 2, tall, LANE), jnp.float32),
            pltpu.VMEM((n_pair, block, depth), bf16),
            pltpu.VMEM((n_pair,) + a_shape, bf16),
            pltpu.VMEM((n_pair, n_pair, block), jnp.float32),
            pltpu.VMEM((n_pair, rank, depth), bf16),
            pltpu.VMEM((n_pair, tall, wide), jnp.float32),
            pltpu.VMEM((n_pair, n_chip, 2 * padded, wide), bf16),
            pltpu.VMEM((2, half, n_chip, 2 * padded, wide), bf16),
            pltpu.VMEM((2, 2 * padded, wide), bf16),
            pltpu.VMEM((2, 2, padded, wide), bf16),
            dma((loads,)), dma((3,)), dma((3,)),
            dma((n_pair,)), dma((n_pair,)),
            dma((extra,)), dma((n_pair,)),
            dma((n_pair,)), dma((n_pair,)),
            dma((n_pair,)), dma((n_pair,)),
            dma((n_pair,)), dma((n_pair,)),
            dma((n_pair, n_aux)), dma((n_aux, n_pair)),
            dma((2, half, n_chip)), dma((2, half, n_chip)),
            dma((3,)), dma((2, 2)),
        ],
        compiler_params=pltpu.CompilerParams(collective_id=0, has_side_effects=True),
    )(x_own, amplitudes, energy, fock, occ, frequency, lmo, neighbours, ranks)


def fits(panels, n_pair, n_aux):
    local_pairs, rank, width = panels.shape
    tiles = width // LANE
    extra = tiles % n_pair
    return (
        local_pairs == 2
        and width % LANE == 0
        and rank % 8 == 0
        and rank % n_aux == 0
        and n_aux % 2 == 0
        and n_pair % 2 == 0
        and 2 * n_pair <= LANE
        and tiles >= n_pair
        and (extra == 0 or n_pair % (2 * extra) == 0)
    )


def body(*operands):
    if fits(operands[0], lax.axis_size("pair"), lax.axis_size("aux")):
        return kernel_body(*operands)
    return plain_body(*operands)


def kernel_body(
    panels,
    amplitudes,
    drive,
    pno_energy,
    occ_energy,
    frequency,
    pair_lmo,
    neighbours,
    pno_ranks,
    fock_off,
):
    local_pairs, rank_dim, aux_width = panels.shape
    coupled = fused_coupling(
        panels.reshape(2 * rank_dim, aux_width), amplitudes, pno_energy, fock_off, occ_energy,
        frequency, pair_lmo.T, neighbours, pno_ranks,
        lax.axis_size("pair"), lax.axis_size("aux"), rank_dim,
    )
    return drive + coupled


def solution(mesh):
    placed = (
        P("pair", None, "aux"),
        P("pair", None, None, None),
        P("pair", None, "aux"),
        P("pair", None),
        P(),
        P(),
        P(),
        P("pair", None),
        P("pair"),
        P(),
    )
    return jax.shard_map(
        body, mesh=mesh, in_specs=placed, out_specs=P("pair", None, "aux"), check_vma=False
    )
```

```python
import functools

import jax
import jax.numpy as jnp
from jax import lax
from jax.experimental import pallas as pl
from jax.experimental.pallas import tpu as pltpu
from jax.sharding import PartitionSpec as P

LANE = 128


def pair_weights(pair_lmo, neighbours, fock_off, first_pair):
    local_pairs = neighbours.shape[0]
    total_pairs = pair_lmo.shape[0]
    lmo_count = fock_off.shape[0]
    lmo_ids = jnp.arange(lmo_count, dtype=jnp.int32)
    own_lmo = lax.dynamic_slice_in_dim(pair_lmo, first_pair, local_pairs, 0)
    own_table = (own_lmo[:, :, None] == lmo_ids[None, None, :]).astype(jnp.float32)
    lmo_table = (pair_lmo[:, :, None] == lmo_ids[None, None, :]).astype(jnp.float32)
    pair_ids = jnp.arange(total_pairs, dtype=jnp.int32)
    onehot = (neighbours[:, :, None] == pair_ids[None, None, :]).astype(jnp.float32)
    fock_rows = jnp.einsum("psl,lm->psm", own_table, fock_off, precision=lax.Precision.HIGHEST)
    near_table = jnp.einsum("pkn,nsl->pksl", onehot, lmo_table)
    values = jnp.sum(fock_rows[:, None, :, :] * near_table, axis=(2, 3))
    weights = jnp.sum(values[:, :, None] * onehot, axis=1).astype(jnp.bfloat16)
    return (weights, own_table)


def plain_body(
    panels,
    amplitudes,
    drive,
    pno_energy,
    occ_energy,
    frequency,
    pair_lmo,
    neighbours,
    pno_ranks,
    fock_off,
):
    local_pairs, rank_dim, aux_width = panels.shape
    total_pairs = pair_lmo.shape[0]
    n_pair = lax.axis_size("pair")
    n_aux = lax.axis_size("aux")
    first_pair = lax.axis_index("pair") * local_pairs
    rows_index = jnp.arange(rank_dim, dtype=jnp.int32)
    keep_rows = rows_index[None, :] < pno_ranks[:, None]
    weights, own_table = pair_weights(pair_lmo, neighbours, fock_off, first_pair)
    weights = lax.all_gather(weights, "pair", axis=0, tiled=True)
    amps = jnp.where(keep_rows[:, :, None, None], jnp.transpose(amplitudes, (0, 2, 1, 3)), 0)
    amps = lax.all_gather(
        amps.reshape(local_pairs * rank_dim, 2 * rank_dim), "pair", axis=0, tiled=True
    )
    masked = jnp.where(keep_rows[:, :, None], panels, jnp.zeros_like(panels))
    slices = lax.all_to_all(
        masked.reshape(local_pairs * rank_dim, aux_width), "pair", 1, 0, tiled=True
    )
    products = jnp.einsum("iq,jq->ij", slices, slices, preferred_element_type=jnp.float32)
    products = products.reshape(total_pairs, rank_dim, total_pairs, rank_dim)
    mixed = (products * weights.astype(jnp.float32)[:, None, :, None]).astype(jnp.bfloat16)
    mixed = mixed.reshape(total_pairs * rank_dim, total_pairs * rank_dim)
    coupled = jnp.dot(mixed, amps, preferred_element_type=jnp.float32).astype(jnp.bfloat16)
    share_width = drive.shape[2]
    coupled = coupled.reshape(total_pairs, rank_dim, 2, rank_dim).transpose(0, 2, 1, 3)
    coupled = coupled.reshape(n_pair, local_pairs, 2, n_aux, share_width).transpose(0, 3, 1, 2, 4)
    coupled = coupled.reshape(n_pair * n_aux, local_pairs, 2, share_width)
    coupled = lax.all_to_all(coupled, ("pair", "aux"), 0, 0, tiled=True)
    coupled_share = jnp.sum(coupled.astype(jnp.float32), axis=0)
    share_start = lax.axis_index("aux") * share_width
    occ_pair = jnp.sum(own_table * occ_energy[None, None, :], axis=(1, 2))
    shift = pno_energy[:, :, None] + pno_energy[:, None, :] - occ_pair[:, None, None]
    shift_flat = lax.dynamic_slice_in_dim(
        shift.reshape(local_pairs, rank_dim * rank_dim), share_start, share_width, 1
    )
    signs = jnp.array([1.0, -1.0], jnp.float32)
    factor = shift_flat[:, None, :] - signs[None, :, None] * frequency[0]
    amp_flat = amplitudes.reshape(local_pairs, 2, rank_dim * rank_dim)
    amp_share = lax.dynamic_slice_in_dim(amp_flat, share_start, share_width, 2).astype(jnp.float32)
    return drive + factor * amp_share + coupled_share


def remote(src, dst, send_sem, recv_sem, pair, aux):
    return pltpu.make_async_remote_copy(
        src_ref=src,
        dst_ref=dst,
        send_sem=send_sem,
        recv_sem=recv_sem,
        device_id=(pair, aux),
        device_id_type=pl.DeviceIdType.MESH,
    )


def kernel(
    n_pair, n_aux, rank, x_hbm, amp_hbm, energy_hbm, fock_hbm,
    occ_hbm, frequency_hbm, lmo_hbm, neighbour_hbm, rank_hbm, out_ref,
    xv, amp_v, energy_v, fock_v, occ_ref, frequency_ref, lmo_ref, neighbour_ref, rank_ref,
    a_ref, term, xb, ab, wt, products, turned_products, left_rows, acc, parts, parts_in, ends, ends_in, nears,
    load_sem, small_sem, local_sem,
    x_send, x_recv, e_send, e_recv, f_send, f_recv, g_send, g_recv,
    a_send, a_recv, b_send, b_recv, p_send, p_recv, q_send, q_recv,
):
    me = lax.axis_index("pair")
    aux = lax.axis_index("aux")
    core = lax.rem(aux, 2)
    chip = aux // 2
    mate = aux + 1 - 2 * core
    n_chip = n_aux // 2
    block = 2 * rank
    tiles = xv.shape[1] // LANE
    base = (tiles // n_pair) * LANE
    extra = tiles % n_pair
    share = a_ref.shape[0] // n_aux
    quarter = rank // n_aux
    padded = ends.shape[1]
    half = n_pair // 2
    near = (me // half) * half
    far = half - near
    spot_me = me - near
    across = far + spot_me

    loads = load_sem.shape[0]
    piece = xv.shape[1] // loads

    def load_x(s):
        lanes = pl.ds(s * piece, piece)
        return pltpu.make_async_copy(x_hbm.at[:, lanes], xv.at[:, lanes], load_sem.at[s])

    smalls = [
        pltpu.make_async_copy(source, target, small_sem.at[s])
        for s, (source, target) in enumerate([
            (amp_hbm, amp_v), (fock_hbm, fock_v), (energy_hbm, energy_v), (occ_hbm, occ_ref),
            (frequency_hbm, frequency_ref), (lmo_hbm, lmo_ref), (neighbour_hbm, neighbour_ref),
            (rank_hbm, rank_ref),
        ])
    ]
    for copy in smalls:
        copy.start()
    for s in range(loads):
        load_x(s).start()

    barrier = pltpu.get_barrier_semaphore()

    def greet(pair, other):
        pl.semaphore_signal(
            barrier, inc=1, device_id=(pair, other), device_id_type=pl.DeviceIdType.MESH
        )

    def near_peer(t):
        return near + lax.rem(spot_me + t, half)

    def far_peer(t):
        return far + lax.rem(spot_me + t, half)

    def row(u):
        return 2 * lax.rem(chip + u, n_chip) + core

    for t in range(half):
        greet(far_peer(t), aux)
    for t in range(1, half):
        greet(near_peer(t), aux)
        for v in range(1, n_aux):
            greet(near_peer(t), lax.rem(aux + v, n_aux))
    for t in range(1, n_aux):
        greet(me, lax.rem(aux + t, n_aux))

    def holder(which, level):
        return half // 2 * (1 + level) + which

    first = base + (LANE if extra else 0)
    lanes = pl.ds(0, base)
    mate_lanes = pl.ds(first, base)
    extra_lanes = pl.ds(base, LANE)
    my_share = pl.ds(pl.multiple_of(aux * share, 16), share)

    def own_cols(peer):
        return xv.at[:, pl.ds(pl.multiple_of(peer * base, LANE), base)]

    def await_bytes(view, send, recv):
        return remote(view, view, send, recv, me, mate)

    def send_a(t):
        peer = near_peer(t) if t else across
        return remote(
            a_ref.at[my_share], ab.at[me, my_share], a_send.at[0], a_recv.at[1 if t else 0], peer, aux
        )

    def pass_a(t):
        rows = ab.at[across, my_share]
        return remote(rows, rows, a_send.at[0], a_recv.at[2], near_peer(t), aux)

    def shares(blocks, count):
        return ab.at[pl.ds(0, blocks), pl.ds(0, count * share)]

    def wait_a(which):
        blocks = half - 1 if which else 1
        await_bytes(shares(blocks, 1), a_send.at[0], a_recv.at[which]).wait_recv()

    def send_x(peer):
        return remote(
            own_cols(peer), xb.at[me, :, lanes], x_send.at[0], x_recv.at[me], peer, aux
        )

    def wait_x(j):
        await_bytes(xb.at[j, :, lanes], x_send.at[0], x_recv.at[j]).wait_recv()

    def wait_f(k):
        await_bytes(xb.at[0, :, mate_lanes], f_send.at[0], f_recv.at[k]).wait_recv()

    def extra_cols(level):
        return xv.at[:, pl.ds(base * n_pair + level * LANE, LANE)]

    def send_e(level):
        return remote(
            extra_cols(level), xb.at[me, :, extra_lanes], e_send.at[level], e_recv.at[0],
            holder(core, level), aux,
        )

    def send_f(j, k):
        return remote(
            xb.at[j, :, lanes], xb.at[j, :, mate_lanes], f_send.at[0], f_recv.at[k], me, mate
        )

    def own_f():
        return remote(
            own_cols(me), xb.at[me, :, mate_lanes], f_send.at[0], f_recv.at[half], me, mate
        )

    def send_g():
        view = xb.at[:, :, extra_lanes]
        return remote(view, view, g_send.at[0], g_recv.at[0], me, mate)

    def send_b(j, u, which):
        rows = ab.at[j, my_share]
        return remote(
            rows, rows, b_send.at[0], b_recv.at[which], me, lax.rem(aux + u, n_aux)
        )

    mine_x = pltpu.make_async_copy(own_cols(me), xb.at[me, :, lanes], local_sem.at[0])
    mine_a = pltpu.make_async_copy(a_ref, ab.at[me], local_sem.at[1])

    def holds(which):
        found = me < 0
        for level in range(extra):
            found = jnp.logical_or(found, holder(which, level) == me)
        return found

    self_holds = holds(core)
    mate_holds = holds(1 - core)
    if extra:
        @pl.when(jnp.logical_not(jnp.logical_or(self_holds, mate_holds)))
        def _():
            xb[:, :, base:first] = jnp.zeros((n_pair, block, LANE), xb.dtype)

    for copy in smalls:
        copy.wait()
    own_amplitudes(rank, me, amp_v, fock_v, lmo_ref, neighbour_ref, rank_ref, a_ref)
    mine_a.start()
    for s in range(loads):
        load_x(s).wait()
    pl.semaphore_wait(barrier, half + half * n_aux - 1)

    for t in range(half):
        send_a(t).start()
    for level in range(extra):
        @pl.when(holder(core, level) != me)
        def _():
            send_e(level).start()

        @pl.when(holder(core, level) == me)
        def _():
            pltpu.make_async_copy(
                extra_cols(level), xb.at[me, :, extra_lanes], local_sem.at[2]
            ).start()
    send_x(near_peer(half // 2)).start()
    level = me // (half // 2)
    inner = jnp.logical_or(level == 1, level == 2)

    @pl.when(inner)
    def _():
        for t in range(half):
            send_x(far_peer(t)).start()

    own_f().start()
    mine_x.start()
    own_term(rank, n_aux, me, aux, amp_v, energy_v, occ_ref, frequency_ref, lmo_ref, term)

    wait_a(0)
    for t in range(1, half):
        pass_a(t).start()
    for u in range(1, n_aux):
        send_b(across, u, 1).start()
    for t in range(1, half):
        if t != half // 2:
            send_x(near_peer(t)).start()

    @pl.when(jnp.logical_not(inner))
    def _():
        for t in range(half):
            send_x(far_peer(t)).start()

    wait_a(1)
    for t in range(1, half):
        for u in range(1, n_aux):
            send_b(near_peer(t), u, 0).start()
    wait_a(2)
    for t in range(1, half):
        for u in range(1, n_aux):
            send_b(far_peer(t), u, 1).start()
    mine_x.wait()
    mine_a.wait()
    if extra:
        @pl.when(self_holds)
        def _():
            pltpu.make_async_copy(
                extra_cols(0), xb.at[me, :, extra_lanes], local_sem.at[2]
            ).wait()
            await_bytes(
                xb.at[pl.ds(0, n_pair - 1), :, extra_lanes], e_send.at[0], e_recv.at[0]
            ).wait_recv()
            send_g().start()

        @pl.when(mate_holds)
        def _():
            send_g().wait_recv()
    for t in range(1, half):
        j = near_peer(half - t)
        wait_x(j)
        send_f(j, half).start()
    def wait_b(which):
        blocks = half if which else half - 1
        await_bytes(shares(blocks, n_aux - 1), b_send.at[0], b_recv.at[which]).wait_recv()

    wait_b(0)
    pair_row = lax.broadcasted_iota(jnp.int32, (LANE, block), 0)
    column = lax.broadcasted_iota(jnp.int32, (LANE, block), 1)

    def spread_weights(side, start):
        rows = [
            ab[start + t, block : block + 16, :LANE].astype(jnp.float32) for t in range(half)
        ]
        rows = [jnp.where(core == 0, r[0:1], r[1:2]) for r in rows]
        rows = rows + [jnp.zeros((half, LANE), jnp.float32)]
        table = jnp.concatenate(rows, axis=0).astype(jnp.bfloat16)
        for j in range(n_pair):
            pick = pair_row == jnp.where(column < rank, 2 * j, 2 * j + 1)
            pick = jnp.where(pick, 1.0, 0.0).astype(jnp.bfloat16)
            wt[side, j] = jnp.dot(table, pick, preferred_element_type=jnp.float32)

    spread_weights(0, near)
    def collect_rows(i, part):
        for side in range(2):
            @pl.when(core == side)
            def _():
                left_rows[i, :, part] = xb[i, side * rank : (side + 1) * rank, part]

    def join(pieces):
        return jnp.concatenate(pieces, axis=0) if len(pieces) > 1 else pieces[0]

    def gram(indices, blocks, part):
        rows = join([left_rows[i, :, part] for i in indices])
        columns = join([xb[j, :, part] for j in blocks])
        return lax.dot_general(
            rows, columns, (((1,), (1,)), ((), ())), preferred_element_type=jnp.float32
        )

    def weight(i, side, j):
        return wt[side, j, pl.ds(i - (far if side else near), 1), :]

    def turned(gram_rows, indices, sides, blocks):
        total = None
        for m, j in enumerate(blocks):
            part = gram_rows[:, m * block : (m + 1) * block]
            scaled = [
                part[k * rank : (k + 1) * rank] * weight(i, side, j)
                for k, (i, side) in enumerate(zip(indices, sides))
            ]
            turn = jnp.dot(
                join(scaled).astype(jnp.bfloat16), ab[j, :block, :],
                preferred_element_type=jnp.float32,
            )
            total = turn if total is None else total + turn
        return total

    def add_rows(turn, indices, fresh=False):
        for k, i in enumerate(indices):
            rows = turn[k * rank : (k + 1) * rank]
            if fresh:
                acc[i, :rank, :] = rows
            else:
                acc[i, :rank, :] += rows

    one = slice(0, first)
    two = slice(first, first + base)
    whole = slice(0, first + base)
    near_all = [near + t for t in range(half)]
    await_bytes(
        xb.at[pl.ds(0, half), :, mate_lanes], f_send.at[0], f_recv.at[half]
    ).wait_recv()
    for t in range(half):
        collect_rows(near_peer(t), whole)
    for t in range(half):
        turn = turned(gram(near_all, [near + t], whole), near_all, [0] * half, [near + t])
        add_rows(turn, near_all, fresh=t == 0)
    wait_b(1)
    spread_weights(1, far)
    def send_p(which, t, v):
        peer = near_peer(t)
        other = lax.rem(aux + v, n_aux)
        i = far_peer(t) if which else peer
        return remote(
            parts.at[i, other], parts_in.at[which, t * n_aux + v], p_send.at[0],
            p_recv.at[which], peer, other,
        )

    hops = [(t, v) for t in range(half) for v in range(n_aux) if t or v]

    def spread(which):
        for t in range(half):
            i = far_peer(t) if which else near_peer(t)
            for k in range(n_aux):
                rows = acc[i, quarter * k : quarter * k + padded, :]
                parts[i, k] = rows.astype(parts.dtype)
            for v in range(n_aux):
                if t or v:
                    send_p(which, t, v).start()

    for k in range(half):
        e = far_peer((half - k) % half)
        earlier = [far_peer((half - m) % half) for m in range(k)]
        blocks = near_all + earlier + [e]
        others = earlier + near_all
        sides = [1] * k + [0] * half
        width = block * len(blocks)
        height = rank * len(others)
        wait_x(e)
        send_f(e, k).start()
        collect_rows(e, one)
        products[:, :width] = gram([e], blocks, one)
        turned_products[:height, :] = gram(others, [e], one)
        wait_f(k)
        collect_rows(e, two)
        full = products[:, :width] + gram([e], blocks, two)
        add_rows(turned(full, [e], [1], blocks), [e], fresh=True)
        if k < half - 1:
            full = turned_products[:height, :] + gram(others, [e], two)
            add_rows(turned(full, others, sides, [e]), others)
        else:
            middle = rank * k
            full = turned_products[:middle, :] + gram(earlier, [e], two)
            add_rows(turned(full, earlier, [1] * k, [e]), earlier)
            spread(1)
            full = turned_products[middle:height, :] + gram(near_all, [e], two)
            add_rows(turned(full, near_all, [0] * half, [e]), near_all)
    spread(0)

    def collect(which):
        i = across if which else me
        same = parts[i, aux].astype(jnp.float32)
        cross = jnp.zeros_like(same)
        await_bytes(
            parts_in.at[which, pl.ds(1, len(hops))], p_send.at[0], p_recv.at[which]
        ).wait_recv()
        for t, v in hops:
            got = parts_in[which, t * n_aux + v].astype(jnp.float32)
            if v % 2 == 0:
                same = same + got
            else:
                cross = cross + got
        return same, cross

    def send_q():
        return remote(ends, ends_in, q_send.at[0], q_recv.at[0], across, aux)

    same, cross = collect(1)
    ends[core] = same.astype(ends.dtype)
    ends[1 - core] = cross.astype(ends.dtype)
    send_q().start()
    same, cross = collect(0)
    nears[core] = same
    nears[1 - core] = cross
    send_q().wait_recv()
    at = lax.broadcasted_iota(jnp.int32, (padded, LANE), 0) + aux * quarter
    for side in range(2):
        total = nears[side] + ends_in[side].astype(jnp.float32)
        for s in range(2):
            part = total[:, s * LANE : (s + 1) * LANE]
            part = jnp.where(at < rank_ref[side], part, 0.0)
            part = part + term[side, s, pl.ds(aux * quarter, padded), :]
            for r in range(quarter):
                out_ref[side, s : s + 1, r * rank : (r + 1) * rank] = part[r : r + 1, :rank]

    await_bytes(shares(2 * half - 1, 1), a_send.at[0], a_recv.at[0]).wait_send()
    await_bytes(
        xb.at[pl.ds(0, n_pair - 1), :, lanes], x_send.at[0], x_recv.at[me]
    ).wait_send()
    await_bytes(xb.at[:, :, lanes], f_send.at[0], f_recv.at[0]).wait_send()
    await_bytes(shares(n_pair - 1, n_aux - 1), b_send.at[0], b_recv.at[0]).wait_send()
    for level in range(extra):
        @pl.when(holder(core, level) != me)
        def _():
            send_e(level).wait_send()
    if extra:
        @pl.when(self_holds)
        def _():
            send_g().wait_send()
    await_bytes(
        parts_in.at[:, pl.ds(1, len(hops))], p_send.at[0], p_recv.at[0]
    ).wait_send()
    send_q().wait_send()


def own_amplitudes(rank, me, amp_v, fock_v, lmo_ref, neighbour_ref, rank_ref, a_ref):
    total_pairs = lmo_ref.shape[1]
    lmo_count = fock_v.shape[0]
    a_ref[...] = jnp.zeros_like(a_ref)
    at = lax.broadcasted_iota(jnp.int32, (rank, rank), 0)
    for p in range(2):
        for s in range(2):
            part = jnp.where(at < rank_ref[p], amp_v[p, s].astype(jnp.float32), 0.0)
            a_ref[p * rank : (p + 1) * rank, s * LANE : s * LANE + rank] = part.astype(a_ref.dtype)
    lane = lax.broadcasted_iota(jnp.int32, (1, LANE), 1)
    level = lax.broadcasted_iota(jnp.int32, (lmo_count, LANE), 0)
    values = 0.0
    for side in range(2):
        where = jnp.full((1, LANE), -1, jnp.int32)
        for n in range(total_pairs):
            where = jnp.where(lane == n, lmo_ref[side, n], where)
        table = jnp.where(level == where, 1.0, 0.0)
        rows = [fock_v[pl.ds(lmo_ref[side, 2 * me + p], 1), :] for p in range(2)]
        rows = jnp.concatenate(rows + [jnp.zeros((6, lmo_count), jnp.float32)], axis=0)
        values = values + jnp.dot(
            rows, table, preferred_element_type=jnp.float32, precision=lax.Precision.HIGHEST
        )
    counts = []
    for p in range(2):
        count = jnp.zeros((1, LANE), jnp.float32)
        for k in range(neighbour_ref.shape[1]):
            count = count + jnp.where(lane == neighbour_ref[p, k], 1.0, 0.0)
        counts.append(count)
    counts = jnp.concatenate(counts + [jnp.zeros((6, LANE), jnp.float32)], axis=0)
    rows = jnp.concatenate([values * counts, jnp.zeros((8, LANE), jnp.float32)], axis=0)
    a_ref[2 * rank : 2 * rank + 16, :LANE] = rows.astype(a_ref.dtype)


def own_term(rank, n_aux, me, aux, amp_v, energy_v, occ_ref, frequency_ref, lmo_ref, term):
    row = lax.broadcasted_iota(jnp.int32, (rank, rank), 0)
    column = lax.broadcasted_iota(jnp.int32, (rank, rank), 1)
    term[...] = jnp.zeros_like(term)
    for p in range(2):
        energy = jnp.broadcast_to(energy_v[p : p + 1, :], (rank, rank))
        own = jnp.sum(jnp.where(row == column, energy, 0.0), axis=1, keepdims=True)
        pair = 2 * me + p
        occ = occ_ref[lmo_ref[0, pair]] + occ_ref[lmo_ref[1, pair]]
        shift = own + energy - occ
        for s in range(2):
            factor = shift - frequency_ref[0] if s == 0 else shift + frequency_ref[0]
            term[p, s, :rank, :rank] = factor * amp_v[p, s].astype(jnp.float32)


def fused_coupling(
    x_own, amplitudes, energy, fock, occ, frequency, lmo, neighbours, ranks, n_pair, n_aux, rank
):
    block = 2 * rank
    tiles = x_own.shape[1] // LANE
    depth = 2 * (tiles // n_pair) * LANE + (LANE if tiles % n_pair else 0)
    n_chip = n_aux // 2
    half = n_pair // 2
    extra = max(tiles % n_pair, 1)
    wide = 2 * LANE
    a_shape = (-(-(block + 16) // (16 * n_aux)) * 16 * n_aux, wide)
    padded = -(-(rank // n_aux) // 16) * 16
    tall = -(-(rank - rank // n_aux + padded) // 8) * 8
    loads = 2 if tiles % 2 == 0 else 1
    dma = pltpu.SemaphoreType.DMA
    bf16 = jnp.bfloat16
    return pl.pallas_call(
        functools.partial(kernel, n_pair, n_aux, rank),
        out_shape=jax.ShapeDtypeStruct((2, 2, rank // n_aux * rank), jnp.float32),
        in_specs=[pl.BlockSpec(memory_space=pl.ANY)] * 9,
        out_specs=pl.BlockSpec(memory_space=pltpu.VMEM),
        scratch_shapes=[
            pltpu.VMEM(x_own.shape, bf16),
            pltpu.VMEM(amplitudes.shape, bf16),
            pltpu.VMEM(energy.shape, jnp.float32),
            pltpu.VMEM(fock.shape, jnp.float32),
            pltpu.SMEM(occ.shape, jnp.float32),
            pltpu.SMEM(frequency.shape, jnp.float32),
            pltpu.SMEM(lmo.shape, jnp.int32),
            pltpu.SMEM(neighbours.shape, jnp.int32),
            pltpu.SMEM(ranks.shape, jnp.int32),
            pltpu.VMEM(a_shape, bf16),
            pltpu.VMEM((2, 2, tall, LANE), jnp.float32),
            pltpu.VMEM((n_pair, block, depth), bf16),
            pltpu.VMEM((n_pair,) + a_shape, bf16),
            pltpu.VMEM((2, n_pair, n_pair, block), jnp.float32),
            pltpu.VMEM((rank, n_pair * block), jnp.float32),
            pltpu.VMEM(((n_pair - 1) * rank, block), jnp.float32),
            pltpu.VMEM((n_pair, rank, depth), bf16),
            pltpu.VMEM((n_pair, tall, wide), jnp.float32),
            pltpu.VMEM((n_pair, n_aux, padded, wide), bf16),
            pltpu.VMEM((2, half * n_aux, padded, wide), bf16),
            pltpu.VMEM((2, padded, wide), bf16),
            pltpu.VMEM((2, padded, wide), bf16),
            pltpu.VMEM((2, padded, wide), jnp.float32),
            dma((loads,)), dma((8,)), dma((3,)),
            dma((1,)), dma((n_pair,)),
            dma((extra,)), dma((1,)),
            dma((1,)), dma((half + 1,)),
            dma((1,)), dma((1,)),
            dma((1,)), dma((3,)),
            dma((1,)), dma((2,)),
            dma((1,)), dma((2,)),
            dma((1,)), dma((1,)),
        ],
        compiler_params=pltpu.CompilerParams(collective_id=0, has_side_effects=True),
    )(x_own, amplitudes, energy, fock, occ, frequency, lmo, neighbours, ranks)


def fits(panels, n_pair, n_aux):
    local_pairs, rank, width = panels.shape
    tiles = width // LANE
    extra = tiles % n_pair
    return (
        local_pairs == 2
        and width % LANE == 0
        and rank % 8 == 0
        and rank % n_aux == 0
        and n_aux % 2 == 0
        and n_pair % 2 == 0
        and 2 * n_pair <= LANE
        and tiles >= n_pair
        and (extra == 0 or n_pair % (2 * extra) == 0)
    )


def body(*operands):
    if fits(operands[0], lax.axis_size("pair"), lax.axis_size("aux")):
        return kernel_body(*operands)
    return plain_body(*operands)


def kernel_body(
    panels,
    amplitudes,
    drive,
    pno_energy,
    occ_energy,
    frequency,
    pair_lmo,
    neighbours,
    pno_ranks,
    fock_off,
):
    local_pairs, rank_dim, aux_width = panels.shape
    coupled = fused_coupling(
        panels.reshape(2 * rank_dim, aux_width), amplitudes, pno_energy, fock_off, occ_energy,
        frequency, pair_lmo.T, neighbours, pno_ranks,
        lax.axis_size("pair"), lax.axis_size("aux"), rank_dim,
    )
    return drive + coupled


def solution(mesh):
    placed = (
        P("pair", None, "aux"),
        P("pair", None, None, None),
        P("pair", None, "aux"),
        P("pair", None),
        P(),
        P(),
        P(),
        P("pair", None),
        P("pair"),
        P(),
    )
    return jax.shard_map(
        body, mesh=mesh, in_specs=placed, out_specs=P("pair", None, "aux"), check_vma=False
    )
```

```python
import functools

import jax
import jax.numpy as jnp
from jax import lax
from jax.experimental import pallas as pl
from jax.experimental.pallas import tpu as pltpu
from jax.sharding import PartitionSpec as P

LANE = 128


def pair_weights(pair_lmo, neighbours, fock_off, first_pair):
    local_pairs = neighbours.shape[0]
    total_pairs = pair_lmo.shape[0]
    lmo_count = fock_off.shape[0]
    lmo_ids = jnp.arange(lmo_count, dtype=jnp.int32)
    own_lmo = lax.dynamic_slice_in_dim(pair_lmo, first_pair, local_pairs, 0)
    own_table = (own_lmo[:, :, None] == lmo_ids[None, None, :]).astype(jnp.float32)
    lmo_table = (pair_lmo[:, :, None] == lmo_ids[None, None, :]).astype(jnp.float32)
    pair_ids = jnp.arange(total_pairs, dtype=jnp.int32)
    onehot = (neighbours[:, :, None] == pair_ids[None, None, :]).astype(jnp.float32)
    fock_rows = jnp.einsum("psl,lm->psm", own_table, fock_off, precision=lax.Precision.HIGHEST)
    near_table = jnp.einsum("pkn,nsl->pksl", onehot, lmo_table)
    values = jnp.sum(fock_rows[:, None, :, :] * near_table, axis=(2, 3))
    weights = jnp.sum(values[:, :, None] * onehot, axis=1).astype(jnp.bfloat16)
    return (weights, own_table)


def plain_body(
    panels,
    amplitudes,
    drive,
    pno_energy,
    occ_energy,
    frequency,
    pair_lmo,
    neighbours,
    pno_ranks,
    fock_off,
):
    local_pairs, rank_dim, aux_width = panels.shape
    total_pairs = pair_lmo.shape[0]
    n_pair = lax.axis_size("pair")
    n_aux = lax.axis_size("aux")
    first_pair = lax.axis_index("pair") * local_pairs
    rows_index = jnp.arange(rank_dim, dtype=jnp.int32)
    keep_rows = rows_index[None, :] < pno_ranks[:, None]
    weights, own_table = pair_weights(pair_lmo, neighbours, fock_off, first_pair)
    weights = lax.all_gather(weights, "pair", axis=0, tiled=True)
    amps = jnp.where(keep_rows[:, :, None, None], jnp.transpose(amplitudes, (0, 2, 1, 3)), 0)
    amps = lax.all_gather(
        amps.reshape(local_pairs * rank_dim, 2 * rank_dim), "pair", axis=0, tiled=True
    )
    masked = jnp.where(keep_rows[:, :, None], panels, jnp.zeros_like(panels))
    slices = lax.all_to_all(
        masked.reshape(local_pairs * rank_dim, aux_width), "pair", 1, 0, tiled=True
    )
    products = jnp.einsum("iq,jq->ij", slices, slices, preferred_element_type=jnp.float32)
    products = products.reshape(total_pairs, rank_dim, total_pairs, rank_dim)
    mixed = (products * weights.astype(jnp.float32)[:, None, :, None]).astype(jnp.bfloat16)
    mixed = mixed.reshape(total_pairs * rank_dim, total_pairs * rank_dim)
    coupled = jnp.dot(mixed, amps, preferred_element_type=jnp.float32).astype(jnp.bfloat16)
    share_width = drive.shape[2]
    coupled = coupled.reshape(total_pairs, rank_dim, 2, rank_dim).transpose(0, 2, 1, 3)
    coupled = coupled.reshape(n_pair, local_pairs, 2, n_aux, share_width).transpose(0, 3, 1, 2, 4)
    coupled = coupled.reshape(n_pair * n_aux, local_pairs, 2, share_width)
    coupled = lax.all_to_all(coupled, ("pair", "aux"), 0, 0, tiled=True)
    coupled_share = jnp.sum(coupled.astype(jnp.float32), axis=0)
    share_start = lax.axis_index("aux") * share_width
    occ_pair = jnp.sum(own_table * occ_energy[None, None, :], axis=(1, 2))
    shift = pno_energy[:, :, None] + pno_energy[:, None, :] - occ_pair[:, None, None]
    shift_flat = lax.dynamic_slice_in_dim(
        shift.reshape(local_pairs, rank_dim * rank_dim), share_start, share_width, 1
    )
    signs = jnp.array([1.0, -1.0], jnp.float32)
    factor = shift_flat[:, None, :] - signs[None, :, None] * frequency[0]
    amp_flat = amplitudes.reshape(local_pairs, 2, rank_dim * rank_dim)
    amp_share = lax.dynamic_slice_in_dim(amp_flat, share_start, share_width, 2).astype(jnp.float32)
    return drive + factor * amp_share + coupled_share


def remote(src, dst, send_sem, recv_sem, pair, aux):
    return pltpu.make_async_remote_copy(
        src_ref=src,
        dst_ref=dst,
        send_sem=send_sem,
        recv_sem=recv_sem,
        device_id=(pair, aux),
        device_id_type=pl.DeviceIdType.MESH,
    )


def kernel(
    n_pair, n_aux, rank, x_hbm, amp_hbm, energy_hbm, fock_hbm,
    occ_hbm, frequency_hbm, lmo_hbm, neighbour_hbm, rank_hbm, out_ref,
    xv, amp_v, energy_v, fock_v, occ_ref, frequency_ref, lmo_ref, neighbour_ref, rank_ref,
    a_ref, term, xb, ab, wt, products, turned_products, left_rows, acc, parts, parts_in, ends, ends_in, nears,
    load_sem, small_sem, local_sem,
    x_send, x_recv, e_send, e_recv, f_send, f_recv, g_send, g_recv,
    a_send, a_recv, b_send, b_recv, p_send, p_recv, q_send, q_recv,
):
    me = lax.axis_index("pair")
    aux = lax.axis_index("aux")
    core = lax.rem(aux, 2)
    chip = aux // 2
    mate = aux + 1 - 2 * core
    n_chip = n_aux // 2
    block = 2 * rank
    tiles = xv.shape[1] // LANE
    base = (tiles // n_pair) * LANE
    extra = tiles % n_pair
    share = a_ref.shape[0] // n_aux
    quarter = rank // n_aux
    padded = ends.shape[1]
    half = n_pair // 2
    near = (me // half) * half
    far = half - near
    spot_me = me - near
    across = far + spot_me

    loads = load_sem.shape[0]
    piece = xv.shape[1] // loads

    def load_x(s):
        lanes = pl.ds(s * piece, piece)
        return pltpu.make_async_copy(x_hbm.at[:, lanes], xv.at[:, lanes], load_sem.at[s])

    barrier = pltpu.get_barrier_semaphore()

    def greet(pair, other):
        pl.semaphore_signal(
            barrier, inc=1, device_id=(pair, other), device_id_type=pl.DeviceIdType.MESH
        )

    def near_peer(t):
        return near + lax.rem(spot_me + t, half)

    def far_peer(t):
        return far + lax.rem(spot_me + t, half)

    turns = [3, 1, 2, 0]

    def partner(t):
        mask = turns[t] if half == len(turns) else t
        return far + jnp.bitwise_xor(spot_me, mask)

    def row(u):
        return 2 * lax.rem(chip + u, n_chip) + core

    for t in range(half):
        greet(far_peer(t), aux)
    for t in range(1, half):
        greet(near_peer(t), aux)
        for v in range(1, n_aux):
            greet(near_peer(t), lax.rem(aux + v, n_aux))
    for t in range(1, n_aux):
        greet(me, lax.rem(aux + t, n_aux))

    smalls = [
        pltpu.make_async_copy(source, target, small_sem.at[s])
        for s, (source, target) in enumerate([
            (amp_hbm, amp_v), (fock_hbm, fock_v), (energy_hbm, energy_v), (occ_hbm, occ_ref),
            (frequency_hbm, frequency_ref), (lmo_hbm, lmo_ref), (neighbour_hbm, neighbour_ref),
            (rank_hbm, rank_ref),
        ])
    ]
    for copy in smalls:
        copy.start()
    for s in range(loads):
        load_x(s).start()

    def holder(which, level):
        return half // 2 * (1 + level) + which

    first = base + (LANE if extra else 0)
    lanes = pl.ds(0, base)
    mate_lanes = pl.ds(first, base)
    extra_lanes = pl.ds(base, LANE)
    my_share = pl.ds(pl.multiple_of(aux * share, 16), share)

    def own_cols(peer):
        return xv.at[:, pl.ds(pl.multiple_of(peer * base, LANE), base)]

    def await_bytes(view, send, recv):
        return remote(view, view, send, recv, me, mate)

    def send_a(t):
        peer = near_peer(t) if t else across
        return remote(
            a_ref.at[my_share], ab.at[me, my_share], a_send.at[0], a_recv.at[1 if t else 0], peer, aux
        )

    def pass_a(t):
        rows = ab.at[across, my_share]
        return remote(rows, rows, a_send.at[0], a_recv.at[2], near_peer(t), aux)

    def shares(blocks, count):
        return ab.at[pl.ds(0, blocks), pl.ds(0, count * share)]

    def wait_a(which):
        blocks = half - 1 if which else 1
        await_bytes(shares(blocks, 1), a_send.at[0], a_recv.at[which]).wait_recv()

    def send_x(peer):
        return remote(
            own_cols(peer), xb.at[me, :, lanes], x_send.at[0], x_recv.at[me], peer, aux
        )

    def wait_x(j):
        await_bytes(xb.at[j, :, lanes], x_send.at[0], x_recv.at[j]).wait_recv()

    def wait_f(k):
        await_bytes(xb.at[0, :, mate_lanes], f_send.at[0], f_recv.at[k]).wait_recv()

    def extra_cols(level):
        return xv.at[:, pl.ds(base * n_pair + level * LANE, LANE)]

    def send_e(level):
        return remote(
            extra_cols(level), xb.at[me, :, extra_lanes], e_send.at[level], e_recv.at[0],
            holder(core, level), aux,
        )

    def send_f(j, k):
        return remote(
            xb.at[j, :, lanes], xb.at[j, :, mate_lanes], f_send.at[0], f_recv.at[k], me, mate
        )

    def own_f():
        return remote(
            own_cols(me), xb.at[me, :, mate_lanes], f_send.at[0], f_recv.at[half], me, mate
        )

    def send_g():
        view = xb.at[:, :, extra_lanes]
        return remote(view, view, g_send.at[0], g_recv.at[0], me, mate)

    def send_b(j, u, which):
        rows = ab.at[j, my_share]
        return remote(
            rows, rows, b_send.at[0], b_recv.at[which], me, lax.rem(aux + u, n_aux)
        )

    mine_x = pltpu.make_async_copy(own_cols(me), xb.at[me, :, lanes], local_sem.at[0])
    mine_a = pltpu.make_async_copy(a_ref, ab.at[me], local_sem.at[1])

    def holds(which):
        found = me < 0
        for level in range(extra):
            found = jnp.logical_or(found, holder(which, level) == me)
        return found

    self_holds = holds(core)
    mate_holds = holds(1 - core)
    if extra:
        @pl.when(jnp.logical_not(jnp.logical_or(self_holds, mate_holds)))
        def _():
            xb[:, :, base:first] = jnp.zeros((n_pair, block, LANE), xb.dtype)

    for copy in smalls:
        copy.wait()
    own_amplitudes(rank, me, amp_v, fock_v, lmo_ref, neighbour_ref, rank_ref, a_ref)
    mine_a.start()
    for s in range(loads):
        load_x(s).wait()
    pl.semaphore_wait(barrier, half + half * n_aux - 1)

    for t in range(half):
        send_a(t).start()
    for level in range(extra):
        @pl.when(holder(core, level) != me)
        def _():
            send_e(level).start()

        @pl.when(holder(core, level) == me)
        def _():
            pltpu.make_async_copy(
                extra_cols(level), xb.at[me, :, extra_lanes], local_sem.at[2]
            ).start()
    send_x(near_peer(half // 2)).start()
    level = me // (half // 2)
    inner = jnp.logical_or(level == 1, level == 2)

    @pl.when(inner)
    def _():
        for t in range(half):
            send_x(partner(t)).start()

    own_f().start()
    mine_x.start()
    own_term(rank, n_aux, me, aux, amp_v, energy_v, occ_ref, frequency_ref, lmo_ref, term)

    wait_a(0)
    for t in range(1, half):
        pass_a(t).start()
    for u in range(1, n_aux):
        send_b(across, u, 1).start()
    for t in range(1, half):
        if t != half // 2:
            send_x(near_peer(t)).start()

    @pl.when(jnp.logical_not(inner))
    def _():
        for t in range(half):
            send_x(partner(t)).start()

    wait_a(1)
    for t in range(1, half):
        for u in range(1, n_aux):
            send_b(near_peer(t), u, 0).start()
    wait_a(2)
    for t in range(1, half):
        for u in range(1, n_aux):
            send_b(far_peer(t), u, 1).start()
    mine_x.wait()
    mine_a.wait()
    if extra:
        @pl.when(self_holds)
        def _():
            pltpu.make_async_copy(
                extra_cols(0), xb.at[me, :, extra_lanes], local_sem.at[2]
            ).wait()
            await_bytes(
                xb.at[pl.ds(0, n_pair - 1), :, extra_lanes], e_send.at[0], e_recv.at[0]
            ).wait_recv()
            send_g().start()

        @pl.when(mate_holds)
        def _():
            send_g().wait_recv()
    for t in range(1, half):
        j = near_peer(half - t)
        wait_x(j)
        send_f(j, half).start()
    def wait_b(which):
        blocks = half if which else half - 1
        await_bytes(shares(blocks, n_aux - 1), b_send.at[0], b_recv.at[which]).wait_recv()

    wait_b(0)
    pair_row = lax.broadcasted_iota(jnp.int32, (LANE, block), 0)
    column = lax.broadcasted_iota(jnp.int32, (LANE, block), 1)

    def spread_weights(side, start):
        rows = [
            ab[start + t, block : block + 16, :LANE].astype(jnp.float32) for t in range(half)
        ]
        rows = [jnp.where(core == 0, r[0:1], r[1:2]) for r in rows]
        rows = rows + [jnp.zeros((half, LANE), jnp.float32)]
        table = jnp.concatenate(rows, axis=0).astype(jnp.bfloat16)
        for j in range(n_pair):
            pick = pair_row == jnp.where(column < rank, 2 * j, 2 * j + 1)
            pick = jnp.where(pick, 1.0, 0.0).astype(jnp.bfloat16)
            wt[side, j] = jnp.dot(table, pick, preferred_element_type=jnp.float32)

    spread_weights(0, near)
    def collect_rows(i, part):
        for side in range(2):
            @pl.when(core == side)
            def _():
                left_rows[i, :, part] = xb[i, side * rank : (side + 1) * rank, part]

    def join(pieces):
        return jnp.concatenate(pieces, axis=0) if len(pieces) > 1 else pieces[0]

    def gram(indices, blocks, part):
        rows = join([left_rows[i, :, part] for i in indices])
        columns = join([xb[j, :, part] for j in blocks])
        return lax.dot_general(
            rows, columns, (((1,), (1,)), ((), ())), preferred_element_type=jnp.float32
        )

    def weight(i, side, j):
        return wt[side, j, pl.ds(i - (far if side else near), 1), :]

    def turned(gram_rows, indices, sides, blocks):
        scaled = []
        for k, (i, side) in enumerate(zip(indices, sides)):
            weights = [weight(i, side, j) for j in blocks]
            weights = jnp.concatenate(weights, axis=1) if len(blocks) > 1 else weights[0]
            scaled.append(gram_rows[k * rank : (k + 1) * rank] * weights)
        return jnp.dot(
            join(scaled).astype(jnp.bfloat16), join([ab[j, :block, :] for j in blocks]),
            preferred_element_type=jnp.float32,
        )

    def add_rows(turn, indices, fresh=False):
        for k, i in enumerate(indices):
            rows = turn[k * rank : (k + 1) * rank]
            if fresh:
                acc[i, :rank, :] = rows
            else:
                acc[i, :rank, :] += rows

    one = slice(0, first)
    two = slice(first, first + base)
    whole = slice(0, first + base)
    near_all = [near + t for t in range(half)]
    await_bytes(
        xb.at[pl.ds(0, half), :, mate_lanes], f_send.at[0], f_recv.at[half]
    ).wait_recv()
    for t in range(half):
        collect_rows(near_peer(t), whole)
    for t in range(half):
        turn = turned(gram(near_all, [near + t], whole), near_all, [0] * half, [near + t])
        add_rows(turn, near_all, fresh=t == 0)
    wait_b(1)
    spread_weights(1, far)
    def send_p(which, t, v):
        peer = near_peer(t)
        other = lax.rem(aux + v, n_aux)
        i = far_peer(t) if which else peer
        return remote(
            parts.at[i, other], parts_in.at[which, t * n_aux + v], p_send.at[which],
            p_recv.at[which], peer, other,
        )

    hops = [(t, v) for t in range(half) for v in range(n_aux) if t or v]

    def spread(which):
        for t in range(half):
            i = far_peer(t) if which else near_peer(t)
            for k in range(n_aux):
                rows = acc[i, quarter * k : quarter * k + padded, :]
                parts[i, k] = rows.astype(parts.dtype)
            if which:
                for v in range(n_aux):
                    if t or v:
                        send_p(which, t, v).start()
        if not which:
            await_bytes(
                parts_in.at[1, pl.ds(1, len(hops))], p_send.at[1], p_recv.at[1]
            ).wait_send()
            for t, v in hops:
                send_p(which, t, v).start()

    for k in range(half):
        e = partner(k)
        earlier = [partner(m) for m in range(k)]
        blocks = near_all + earlier + [e]
        prompt = k < half - 2
        others = earlier + (near_all if prompt else [])
        sides = [1] * k + ([0] * half if prompt else [])
        width = block * len(blocks)
        height = rank * len(others)
        wait_x(e)
        send_f(e, k).start()
        collect_rows(e, one)
        products[:, :width] = gram([e], blocks, one)
        if others:
            turned_products[:height, :] = gram(others, [e], one)
        wait_f(k)
        collect_rows(e, two)
        full = products[:, :width] + gram([e], blocks, two)
        add_rows(turned(full, [e], [1], blocks), [e], fresh=True)
        if others:
            full = turned_products[:height, :] + gram(others, [e], two)
            add_rows(turned(full, others, sides, [e]), others)
    spread(1)
    held = [partner(m) for m in range(half - 2, half)]
    add_rows(turned(gram(near_all, held, whole), near_all, [0] * half, held), near_all)
    spread(0)

    def collect(which):
        i = across if which else me
        same = parts[i, aux].astype(jnp.float32)
        cross = jnp.zeros_like(same)
        await_bytes(
            parts_in.at[which, pl.ds(1, len(hops))], p_send.at[which], p_recv.at[which]
        ).wait_recv()
        for t, v in hops:
            got = parts_in[which, t * n_aux + v].astype(jnp.float32)
            if v % 2 == 0:
                same = same + got
            else:
                cross = cross + got
        return same, cross

    def send_q():
        return remote(ends, ends_in, q_send.at[0], q_recv.at[0], across, aux)

    same, cross = collect(1)
    ends[core] = same.astype(ends.dtype)
    ends[1 - core] = cross.astype(ends.dtype)
    send_q().start()
    same, cross = collect(0)
    nears[core] = same
    nears[1 - core] = cross
    send_q().wait_recv()
    at = lax.broadcasted_iota(jnp.int32, (padded, LANE), 0) + aux * quarter
    for side in range(2):
        total = nears[side] + ends_in[side].astype(jnp.float32)
        for s in range(2):
            part = total[:, s * LANE : (s + 1) * LANE]
            part = jnp.where(at < rank_ref[side], part, 0.0)
            part = part + term[side, s, pl.ds(aux * quarter, padded), :]
            for r in range(quarter):
                out_ref[side, s : s + 1, r * rank : (r + 1) * rank] = part[r : r + 1, :rank]

    await_bytes(shares(2 * half - 1, 1), a_send.at[0], a_recv.at[0]).wait_send()
    await_bytes(
        xb.at[pl.ds(0, n_pair - 1), :, lanes], x_send.at[0], x_recv.at[me]
    ).wait_send()
    await_bytes(xb.at[:, :, lanes], f_send.at[0], f_recv.at[0]).wait_send()
    await_bytes(shares(n_pair - 1, n_aux - 1), b_send.at[0], b_recv.at[0]).wait_send()
    for level in range(extra):
        @pl.when(holder(core, level) != me)
        def _():
            send_e(level).wait_send()
    if extra:
        @pl.when(self_holds)
        def _():
            send_g().wait_send()
    await_bytes(
        parts_in.at[0, pl.ds(1, len(hops))], p_send.at[0], p_recv.at[0]
    ).wait_send()
    send_q().wait_send()


def own_amplitudes(rank, me, amp_v, fock_v, lmo_ref, neighbour_ref, rank_ref, a_ref):
    total_pairs = lmo_ref.shape[1]
    lmo_count = fock_v.shape[0]
    a_ref[...] = jnp.zeros_like(a_ref)
    at = lax.broadcasted_iota(jnp.int32, (rank, rank), 0)
    for p in range(2):
        for s in range(2):
            part = jnp.where(at < rank_ref[p], amp_v[p, s].astype(jnp.float32), 0.0)
            a_ref[p * rank : (p + 1) * rank, s * LANE : s * LANE + rank] = part.astype(a_ref.dtype)
    lane = lax.broadcasted_iota(jnp.int32, (1, LANE), 1)
    level = lax.broadcasted_iota(jnp.int32, (lmo_count, LANE), 0)
    values = 0.0
    for side in range(2):
        where = jnp.full((1, LANE), -1, jnp.int32)
        for n in range(total_pairs):
            where = jnp.where(lane == n, lmo_ref[side, n], where)
        table = jnp.where(level == where, 1.0, 0.0)
        rows = [fock_v[pl.ds(lmo_ref[side, 2 * me + p], 1), :] for p in range(2)]
        rows = jnp.concatenate(rows + [jnp.zeros((6, lmo_count), jnp.float32)], axis=0)
        values = values + jnp.dot(
            rows, table, preferred_element_type=jnp.float32, precision=lax.Precision.HIGHEST
        )
    counts = []
    for p in range(2):
        count = jnp.zeros((1, LANE), jnp.float32)
        for k in range(neighbour_ref.shape[1]):
            count = count + jnp.where(lane == neighbour_ref[p, k], 1.0, 0.0)
        counts.append(count)
    counts = jnp.concatenate(counts + [jnp.zeros((6, LANE), jnp.float32)], axis=0)
    rows = jnp.concatenate([values * counts, jnp.zeros((8, LANE), jnp.float32)], axis=0)
    a_ref[2 * rank : 2 * rank + 16, :LANE] = rows.astype(a_ref.dtype)


def own_term(rank, n_aux, me, aux, amp_v, energy_v, occ_ref, frequency_ref, lmo_ref, term):
    row = lax.broadcasted_iota(jnp.int32, (rank, rank), 0)
    column = lax.broadcasted_iota(jnp.int32, (rank, rank), 1)
    term[...] = jnp.zeros_like(term)
    for p in range(2):
        energy = jnp.broadcast_to(energy_v[p : p + 1, :], (rank, rank))
        own = jnp.sum(jnp.where(row == column, energy, 0.0), axis=1, keepdims=True)
        pair = 2 * me + p
        occ = occ_ref[lmo_ref[0, pair]] + occ_ref[lmo_ref[1, pair]]
        shift = own + energy - occ
        for s in range(2):
            factor = shift - frequency_ref[0] if s == 0 else shift + frequency_ref[0]
            term[p, s, :rank, :rank] = factor * amp_v[p, s].astype(jnp.float32)


def fused_coupling(
    x_own, amplitudes, energy, fock, occ, frequency, lmo, neighbours, ranks, n_pair, n_aux, rank
):
    block = 2 * rank
    tiles = x_own.shape[1] // LANE
    depth = 2 * (tiles // n_pair) * LANE + (LANE if tiles % n_pair else 0)
    n_chip = n_aux // 2
    half = n_pair // 2
    extra = max(tiles % n_pair, 1)
    wide = 2 * LANE
    a_shape = (-(-(block + 16) // (16 * n_aux)) * 16 * n_aux, wide)
    padded = -(-(rank // n_aux) // 16) * 16
    tall = -(-(rank - rank // n_aux + padded) // 8) * 8
    loads = 2 if tiles % 2 == 0 else 1
    dma = pltpu.SemaphoreType.DMA
    bf16 = jnp.bfloat16
    return pl.pallas_call(
        functools.partial(kernel, n_pair, n_aux, rank),
        out_shape=jax.ShapeDtypeStruct((2, 2, rank // n_aux * rank), jnp.float32),
        in_specs=[pl.BlockSpec(memory_space=pl.ANY)] * 9,
        out_specs=pl.BlockSpec(memory_space=pltpu.VMEM),
        scratch_shapes=[
            pltpu.VMEM(x_own.shape, bf16),
            pltpu.VMEM(amplitudes.shape, bf16),
            pltpu.VMEM(energy.shape, jnp.float32),
            pltpu.VMEM(fock.shape, jnp.float32),
            pltpu.SMEM(occ.shape, jnp.float32),
            pltpu.SMEM(frequency.shape, jnp.float32),
            pltpu.SMEM(lmo.shape, jnp.int32),
            pltpu.SMEM(neighbours.shape, jnp.int32),
            pltpu.SMEM(ranks.shape, jnp.int32),
            pltpu.VMEM(a_shape, bf16),
            pltpu.VMEM((2, 2, tall, LANE), jnp.float32),
            pltpu.VMEM((n_pair, block, depth), bf16),
            pltpu.VMEM((n_pair,) + a_shape, bf16),
            pltpu.VMEM((2, n_pair, n_pair, block), jnp.float32),
            pltpu.VMEM((rank, n_pair * block), jnp.float32),
            pltpu.VMEM(((n_pair - 1) * rank, block), jnp.float32),
            pltpu.VMEM((n_pair, rank, depth), bf16),
            pltpu.VMEM((n_pair, tall, wide), jnp.float32),
            pltpu.VMEM((n_pair, n_aux, padded, wide), bf16),
            pltpu.VMEM((2, half * n_aux, padded, wide), bf16),
            pltpu.VMEM((2, padded, wide), bf16),
            pltpu.VMEM((2, padded, wide), bf16),
            pltpu.VMEM((2, padded, wide), jnp.float32),
            dma((loads,)), dma((8,)), dma((3,)),
            dma((1,)), dma((n_pair,)),
            dma((extra,)), dma((1,)),
            dma((1,)), dma((half + 1,)),
            dma((1,)), dma((1,)),
            dma((1,)), dma((3,)),
            dma((1,)), dma((2,)),
            dma((2,)), dma((2,)),
            dma((1,)), dma((1,)),
        ],
        compiler_params=pltpu.CompilerParams(collective_id=0, has_side_effects=True),
    )(x_own, amplitudes, energy, fock, occ, frequency, lmo, neighbours, ranks)


def fits(panels, n_pair, n_aux):
    local_pairs, rank, width = panels.shape
    tiles = width // LANE
    extra = tiles % n_pair
    return (
        local_pairs == 2
        and width % LANE == 0
        and rank % 8 == 0
        and rank % n_aux == 0
        and n_aux % 2 == 0
        and n_pair >= 8
        and n_pair & (n_pair - 1) == 0
        and rank <= LANE
        and extra <= 2
        and 2 * n_pair <= LANE
        and tiles >= n_pair
        and (extra == 0 or n_pair % (2 * extra) == 0)
    )


def body(*operands):
    if fits(operands[0], lax.axis_size("pair"), lax.axis_size("aux")):
        return kernel_body(*operands)
    return plain_body(*operands)


def kernel_body(
    panels,
    amplitudes,
    drive,
    pno_energy,
    occ_energy,
    frequency,
    pair_lmo,
    neighbours,
    pno_ranks,
    fock_off,
):
    local_pairs, rank_dim, aux_width = panels.shape
    coupled = fused_coupling(
        panels.reshape(2 * rank_dim, aux_width), amplitudes, pno_energy, fock_off, occ_energy,
        frequency, pair_lmo.T, neighbours, pno_ranks,
        lax.axis_size("pair"), lax.axis_size("aux"), rank_dim,
    )
    return drive + coupled


def solution(mesh):
    placed = (
        P("pair", None, "aux"),
        P("pair", None, None, None),
        P("pair", None, "aux"),
        P("pair", None),
        P(),
        P(),
        P(),
        P("pair", None),
        P("pair"),
        P(),
    )
    return jax.shard_map(
        body, mesh=mesh, in_specs=placed, out_specs=P("pair", None, "aux"), check_vma=False
    )
```
